8 devices in a mesh: dp: 2 (over z, y), ep: 4 (over x, core).
Axes of the slice: x: 2, y: 2, z: 1, core: 2. Of those that a mesh axis runs over, the one named last changes fastest.
Arguments:
- x_tok: bfloat16 [16, 1024, 2048], P(('dp', 'ep')), parts along dimension 0
- w_query: bfloat16 [2048, 16, 128], P('ep')
- w_key: bfloat16 [2048, 16, 128], P('ep')
- w_value: bfloat16 [2048, 16, 128], P('ep')
- w_out: bfloat16 [2048, 2048], P('ep')
- w_router: float32 [2048, 64], replicated
- w_gate: bfloat16 [64, 2048, 1408], P('ep')
- w_up: bfloat16 [64, 2048, 1408], P('ep')
- w_down: bfloat16 [64, 1408, 2048], P('ep')
- ws_gate: bfloat16 [2048, 2816], P('ep')
- ws_up: bfloat16 [2048, 2816], P('ep')
- ws_down: bfloat16 [2816, 2048], P('ep')
- expert_ids: int32 [16, 1024, 6], P(('dp', 'ep')), parts along dimension 0
Outputs:
- output: bfloat16 [16, 1024, 2048], P(('dp', 'ep')), parts along dimension 0
There are 2 independent parts. The reference program is written for one: setup_inputs(seed, part) draws one part's arguments, and reference() takes and returns one part's arrays. A program takes and returns all parts, laid end to end along the dimension named above; an argument that names none is the same for every part.
All inputs are finite; a program needn't handle non-finite values.
Results may differ from the reference program's by a relative error of at most 0.0136838.
Values are sent between devices in bfloat16 or wider.
A program may use at most 1.25 GiB of HBM per device.

```python
import jax
import jax.numpy as jnp
import numpy as np
from jax import lax

SEQS_DEV = 2
SEQ = 1024
GROUP = 4
D = 2048
HEADS = 16
HEAD = 128
EXPERTS = 64
TOP = 6
FF = 1408
FFS = 2816
CAP = 384
NHOT = 8

EPSILON = 1e-6
TOK_DEV = SEQS_DEV * SEQ
TOKENS = GROUP * TOK_DEV
N_SEQS = GROUP * SEQS_DEV
WIDTH = HEADS * HEAD


def rms_norm(values):
    as_f32 = values.astype(jnp.float32)
    return as_f32 * lax.rsqrt(jnp.mean(as_f32 * as_f32, axis=-1, keepdims=True) + EPSILON)


def swiglu_ffn(row_block, gate_w, up_w, down_w):
    gate_act = jnp.dot(row_block, gate_w, preferred_element_type=jnp.float32)
    up_act = jnp.dot(row_block, up_w, preferred_element_type=jnp.float32)
    middle = (jax.nn.silu(gate_act) * up_act).astype(jnp.bfloat16)
    return jnp.dot(middle, down_w, preferred_element_type=jnp.float32).astype(jnp.bfloat16)


def routing_table():
    rest_count = TOK_DEV * TOP - NHOT * CAP
    cold_count = EXPERTS - NHOT
    run_counts = np.concatenate([np.full(NHOT, CAP), rest_count // cold_count + (np.arange(cold_count) < rest_count % cold_count)])
    return jnp.asarray(np.repeat(np.arange(EXPERTS), run_counts), dtype=jnp.int32)


def device_routing(dev_key, run_ids):
    label_key, order_key = jax.random.split(dev_key)
    labels = jax.random.permutation(label_key, EXPERTS)
    shuffle = jax.random.permutation(order_key, TOK_DEV)
    table = labels[run_ids].reshape(TOP, TOK_DEV).T
    return table[shuffle]


def setup_inputs(seed: int = 0, part: int = 0) -> dict:
    root_key = jax.random.key(seed)
    part_key = jax.random.fold_in(root_key, part)
    tok_key, route_key = jax.random.split(part_key)
    weight_keys = jax.random.split(root_key, 10)

    def gauss(key_w, shape_w, scale):
        return (jax.random.normal(key_w, shape_w, jnp.float32) * scale).astype(jnp.bfloat16)

    run_ids = routing_table()

    def draw_device(dev_key):
        return device_routing(dev_key, run_ids)

    dev_keys = jax.random.split(route_key, GROUP)
    expert_ids = jax.vmap(draw_device)(dev_keys).reshape(N_SEQS, SEQ, TOP)
    return {
        'x_tok': jax.random.normal(tok_key, (N_SEQS, SEQ, D), jnp.float32).astype(jnp.bfloat16),
        'w_query': gauss(weight_keys[0], (D, HEADS, HEAD), 2.0 * D ** -0.5),
        'w_key': gauss(weight_keys[1], (D, HEADS, HEAD), D ** -0.5),
        'w_value': gauss(weight_keys[2], (D, HEADS, HEAD), D ** -0.5),
        'w_out': gauss(weight_keys[3], (WIDTH, D), 2.0 * WIDTH ** -0.5),
        'w_router': jax.random.normal(weight_keys[4], (D, EXPERTS), jnp.float32) * D ** -0.5,
        'w_gate': gauss(weight_keys[5], (EXPERTS, D, FF), D ** -0.5),
        'w_up': gauss(weight_keys[6], (EXPERTS, D, FF), D ** -0.5),
        'w_down': gauss(weight_keys[7], (EXPERTS, FF, D), 2.0 * FF ** -0.5),
        'ws_gate': gauss(weight_keys[8], (D, FFS), D ** -0.5),
        'ws_up': gauss(weight_keys[9], (D, FFS), D ** -0.5),
        'ws_down': gauss(jax.random.fold_in(root_key, 11), (FFS, D), FFS ** -0.5),
        'expert_ids': expert_ids,
    }


def reference(x_tok, w_query, w_key, w_value, w_out, w_router, w_gate, w_up, w_down, ws_gate, ws_up, ws_down, expert_ids):
    normed = rms_norm(x_tok).astype(jnp.bfloat16).reshape(TOKENS, D)

    def project(weight):
        return jnp.dot(normed, weight.reshape(D, WIDTH), preferred_element_type=jnp.float32).astype(jnp.bfloat16).reshape(N_SEQS, SEQ, HEADS, HEAD)

    queries = project(w_query)
    keys_all = project(w_key)
    vals_all = project(w_value)
    causal = jnp.arange(SEQ)[:, None] >= jnp.arange(SEQ)[None, :]

    def one_seq(seq_block):
        query_blk, key_blk, value_blk = seq_block
        scores = jnp.einsum('qhe,khe->hqk', query_blk.astype(jnp.float32), key_blk.astype(jnp.float32)) * (HEAD ** -0.5)
        attn_probs = jax.nn.softmax(jnp.where(causal[None], scores, -1e30), axis=-1).astype(jnp.bfloat16)
        return jnp.einsum('hqk,khe->qhe', attn_probs.astype(jnp.float32), value_blk.astype(jnp.float32)).astype(jnp.bfloat16)

    attended = lax.map(one_seq, (queries, keys_all, vals_all))
    attn_out = jnp.dot(attended.reshape(TOKENS, WIDTH), w_out, preferred_element_type=jnp.float32).astype(jnp.bfloat16)
    residual = (x_tok.reshape(TOKENS, D).astype(jnp.float32) + attn_out.astype(jnp.float32)).astype(jnp.bfloat16)

    hidden = rms_norm(residual)
    logits = jnp.dot(hidden, w_router, preferred_element_type=jnp.float32)
    tok_ids = expert_ids.reshape(TOKENS, TOP)
    gate_probs = jax.nn.softmax(jnp.take_along_axis(logits, tok_ids, axis=1), axis=-1)
    moe_in = hidden.astype(jnp.bfloat16)

    flat_ids = tok_ids.reshape(-1)
    n_assign = TOKENS * TOP
    sort_order = jnp.argsort(flat_ids, stable=True)
    expert_counts = jnp.bincount(flat_ids, length=EXPERTS)
    expert_starts = jnp.cumsum(expert_counts) - expert_counts
    slot_count = GROUP * CAP
    flat_gates = gate_probs.reshape(-1)

    def one_expert(running, piece):
        gate_w, up_w, down_w, start_at, count_of = piece
        slot_picks = jnp.minimum(start_at + jnp.arange(slot_count), n_assign - 1)
        assign_ids = sort_order[slot_picks]
        slot_gate = jnp.where(jnp.arange(slot_count) < count_of, flat_gates[assign_ids], 0.0)
        slot_token = assign_ids // TOP
        outputs = swiglu_ffn(moe_in[slot_token], gate_w, up_w, down_w)
        running = running.at[slot_token].add(slot_gate[:, None] * outputs.astype(jnp.float32))
        return running, None

    routed, unused = lax.scan(one_expert, jnp.zeros((TOKENS, D), jnp.float32), (w_gate, w_up, w_down, expert_starts, expert_counts))
    shared = swiglu_ffn(moe_in, ws_gate, ws_up, ws_down)
    y_out = (residual.astype(jnp.float32) + routed + shared.astype(jnp.float32)).astype(jnp.bfloat16)
    return y_out.reshape(N_SEQS, SEQ, D)
```

```python
import functools
import jax
import jax.numpy as jnp
from jax import lax
from jax.experimental import pallas as pl
from jax.experimental.pallas import tpu as pltpu
from jax.sharding import PartitionSpec as P

ROWS = 256
SUB = 16
LANES = 128


def expert_kernel(toks, bounds, gates, half_a, half_b, wg, wu, wd, out_a, out_b, tokens_v, sums, stage, rows_b, mid, tok_s, gate_s, sem_in, sem_out, *, n_half, n_src):
    e = pl.program_id(0)
    n_exp = pl.num_programs(0)
    n_tok = 2 * n_half
    ff = wg.shape[2]
    d_model = wd.shape[2]

    @pl.when(e == 0)
    def _():
        ca = pltpu.make_async_copy(half_a, tokens_v.at[pl.ds(0, n_half)], sem_in.at[0])
        cb = pltpu.make_async_copy(half_b, tokens_v.at[pl.ds(n_half, n_half)], sem_in.at[1])
        ca.start()
        cb.start()

        def zero(i, _):
            sums[pl.ds(i * 8, 8)] = jnp.zeros((8, SUB, LANES), jnp.float32)
            return 0
        lax.fori_loop(0, (n_tok + 8) // 8, zero, 0)
        ca.wait()
        cb.wait()

    start_a = bounds[4 * e]
    count_a = bounds[4 * e + 1]
    start_b = bounds[4 * e + 2] + n_src - count_a
    total = count_a + bounds[4 * e + 3]

    def block(b, _):
        base = b * ROWS
        left = jnp.minimum(total - base, ROWS)
        groups = (left + 7) // 8

        def gather(i, _):
            for j in range(8):
                r = i * 8 + j
                row = base + r
                slot = row + jnp.where(row < count_a, start_a, start_b)
                key = toks[slot]
                tok = key >> 3
                stage[pl.ds(pl.multiple_of(r * SUB, SUB), SUB), :] = tokens_v[tok].astype(jnp.float32)
                ok = row < total
                tok_s[r] = jnp.where(ok, tok, n_tok)
                gate_s[r] = gates[key]
            return 0
        lax.fori_loop(0, groups, gather, 0)
        for k in range(SUB):
            rows_b[:, k * LANES:(k + 1) * LANES] = stage[pl.ds(k, ROWS, stride=SUB), :].astype(jnp.bfloat16)
        for c in range(ff // LANES):
            w = jnp.concatenate([wg[0, :, c * LANES:(c + 1) * LANES], wu[0, :, c * LANES:(c + 1) * LANES]], axis=1)
            gu = jnp.dot(rows_b[...], w, preferred_element_type=jnp.float32)
            g = gu[:, :LANES]
            mid[:, c * LANES:(c + 1) * LANES] = (g * jax.nn.sigmoid(g) * gu[:, LANES:]).astype(jnp.bfloat16)
        for c in range(d_model // 256):
            o = jnp.dot(mid[...], wd[0, :, c * 256:(c + 1) * 256], preferred_element_type=jnp.float32)
            o = o.astype(jnp.bfloat16).astype(jnp.float32)
            stage[pl.ds(2 * c, ROWS, stride=SUB), :] = o[:, :LANES]
            stage[pl.ds(2 * c + 1, ROWS, stride=SUB), :] = o[:, LANES:]

        def scatter(i, _):
            toks8 = [tok_s[i * 8 + j] for j in range(8)]
            old = [sums[t] for t in toks8]
            new = [old[j] + gate_s[i * 8 + j] * stage[pl.ds(pl.multiple_of((i * 8 + j) * SUB, SUB), SUB), :] for j in range(8)]
            for j in range(8):
                sums[toks8[j]] = new[j]
            return 0
        lax.fori_loop(0, groups, scatter, 0)
        return 0

    lax.fori_loop(0, (total + ROWS - 1) // ROWS, block, 0)

    @pl.when(e == n_exp - 1)
    def _():
        ca = pltpu.make_async_copy(sums.at[pl.ds(0, n_half)], out_a, sem_out.at[0])
        cb = pltpu.make_async_copy(sums.at[pl.ds(n_half, n_half)], out_b, sem_out.at[1])
        ca.start()
        cb.start()
        ca.wait()
        cb.wait()


def expert_pass(toks, bounds, gates, half_a, half_b, wg, wu, wd, n_src, name):
    n_half = half_a.shape[0]
    n_exp, d_model, ff = wg.shape
    w_in = lambda e, *_: (e, 0, 0)
    any_spec = pl.BlockSpec(memory_space=pl.ANY)
    return pl.pallas_call(
        functools.partial(expert_kernel, n_half=n_half, n_src=n_src),
        grid_spec=pltpu.PrefetchScalarGridSpec(
            num_scalar_prefetch=3,
            grid=(n_exp,),
            in_specs=[any_spec, any_spec,
                      pl.BlockSpec((1, d_model, ff), w_in), pl.BlockSpec((1, d_model, ff), w_in), pl.BlockSpec((1, ff, d_model), w_in)],
            out_specs=[any_spec, any_spec],
            scratch_shapes=[
                pltpu.VMEM((2 * n_half, SUB, LANES), jnp.bfloat16),
                pltpu.VMEM((2 * n_half + 8, SUB, LANES), jnp.float32),
                pltpu.VMEM((ROWS * SUB, LANES), jnp.float32),
                pltpu.VMEM((ROWS, d_model), jnp.bfloat16),
                pltpu.VMEM((ROWS, ff), jnp.bfloat16),
                pltpu.SMEM((ROWS,), jnp.int32),
                pltpu.SMEM((ROWS,), jnp.float32),
                pltpu.SemaphoreType.DMA((2,)),
                pltpu.SemaphoreType.DMA((2,)),
            ],
        ),
        out_shape=[jax.ShapeDtypeStruct((n_half, SUB, LANES), jnp.float32)] * 2,
        compiler_params=pltpu.CompilerParams(vmem_limit_bytes=67043328, dimension_semantics=("arbitrary",)),
        cost_estimate=pl.CostEstimate(flops=2 * 3 * 4096 * d_model * ff, bytes_accessed=n_exp * 3 * d_model * ff * 2, transcendentals=0),
        name=name,
    )(toks, bounds, gates, half_a, half_b, wg, wu, wd)


def attention_kernel(q_ref, k_ref, v_ref, o_ref, *, scale):
    seq = q_ref.shape[0]
    tile = 256
    for i in range(seq // tile):
        span = (i + 1) * tile
        q = q_ref[i * tile:span, :]
        s = lax.dot_general(q, k_ref[:span, :], (((1,), (1,)), ((), ())), preferred_element_type=jnp.float32) * scale
        row = lax.broadcasted_iota(jnp.int32, (tile, span), 0) + i * tile
        col = lax.broadcasted_iota(jnp.int32, (tile, span), 1)
        s = jnp.where(row >= col, s, -1e30)
        p = jnp.exp(s - jnp.max(s, axis=-1, keepdims=True))
        p = (p * (1.0 / jnp.sum(p, axis=-1, keepdims=True))).astype(jnp.bfloat16)
        o_ref[i * tile:span, :] = jnp.dot(p, v_ref[:span, :], preferred_element_type=jnp.float32).astype(jnp.bfloat16)


def attention(q, k, v, seq_index, seq, head):
    width = q.shape[1]
    spec = pl.BlockSpec((seq, head), lambda h: (seq_index, h))
    return pl.pallas_call(
        functools.partial(attention_kernel, scale=head ** -0.5),
        grid=(width // head,),
        in_specs=[spec] * 3,
        out_specs=pl.BlockSpec((seq, head), lambda h: (0, h)),
        out_shape=jax.ShapeDtypeStruct((seq, width), jnp.bfloat16),
        compiler_params=pltpu.CompilerParams(dimension_semantics=("arbitrary",)),
        cost_estimate=pl.CostEstimate(flops=8 * seq * seq * width, bytes_accessed=8 * seq * width, transcendentals=0),
        name="attention",
    )(q, k, v)


EPSILON = 1e-6
X_SWAP = [(0, 2), (1, 3), (2, 0), (3, 1)]
CORE_SWAP = [(0, 1), (1, 0), (2, 3), (3, 2)]
ROW_SWAP = [(0, 1), (1, 0)]


def rms_norm(values):
    as_f32 = values.astype(jnp.float32)
    return as_f32 * lax.rsqrt(jnp.mean(as_f32 * as_f32, axis=-1, keepdims=True) + EPSILON)


def over_x(value):
    return lax.ppermute(value, "ep", X_SWAP)


def over_core(value):
    return lax.ppermute(value, "ep", CORE_SWAP)


def gather_weight(shard, axis):
    me, row = lax.axis_index("ep"), lax.axis_index("dp")
    depth = shard.shape[0]
    half = shard.shape[axis] // 2
    mine = over_x(lax.dynamic_slice_in_dim(shard, row * half, half, axis))
    other = lax.ppermute(mine, "dp", ROW_SWAP)
    pieces = [(me, 0, shard), (me ^ 2, row, mine), (me ^ 2, 1 - row, other)]
    pieces += [(owner ^ 1, part, over_core(piece)) for owner, part, piece in pieces]
    whole = jnp.zeros((4 * depth, shard.shape[1]), shard.dtype)
    for owner, part, piece in pieces:
        at = [owner * depth, jnp.int32(0)]
        at[axis] = at[axis] + part * half
        whole = lax.dynamic_update_slice(whole, piece, at)
    return whole


def route_plan(ids, n_exp, seq):
    n_tok, top = ids.shape
    key = (ids << 14) | (lax.broadcasted_iota(jnp.int32, ids.shape, 0) << 3) | lax.broadcasted_iota(jnp.int32, ids.shape, 1)
    key = lax.sort(key.reshape(-1))
    edge = jnp.arange(2 * n_exp + 1, dtype=jnp.int32)
    edge = ((edge >> 1) << 14) | ((edge & 1) * seq << 3)
    begin = jnp.sum((key[None, :] < edge[:, None]).astype(jnp.int32), axis=1)
    return key, begin


def local_layer(x_loc, q_shard, k_shard, v_shard, o_shard, w_router, w_gate, w_up, w_down, sgate_shard, sup_shard, sdown_shard, ids_loc):
    n_seq, seq, d_model = x_loc.shape
    head = q_shard.shape[2]
    n_tok = n_seq * seq
    top = ids_loc.shape[-1]
    n_loc = w_gate.shape[0]
    n_exp = 4 * n_loc
    me = lax.axis_index("ep")

    flat = lambda w: w.reshape(w.shape[0], -1)
    w_q, w_k, w_v, w_o = [gather_weight(flat(w), 0) for w in (q_shard, k_shard, v_shard, o_shard)]

    ids = ids_loc.reshape(n_tok, top)
    key, begin = route_plan(ids, n_exp, seq)
    n_key = n_tok * top
    plans = lax.all_gather(jnp.concatenate([key, begin]), "ep", axis=0)

    def bounds_of(plan, s):
        local = lax.dynamic_slice_in_dim(plan, n_key + 2 * n_loc * me, 2 * n_loc + 1)
        lo = local[s:s + 2 * n_loc:2]
        hi = local[s + 1:s + 1 + 2 * n_loc:2]
        return lo, hi - lo

    def plan_of(own_a, own_b, s):
        a, b = plans[own_a], plans[own_b]
        ka = a[:n_key] & (8 * seq - 1)
        kb = (b[:n_key] & (8 * seq - 1)) | (8 * seq)
        toks = jnp.concatenate([ka, kb, jnp.zeros((ROWS,), jnp.int32)])
        return toks, jnp.stack([*bounds_of(a, s), *bounds_of(b, s)], axis=1).reshape(-1)

    x_flat = x_loc.reshape(n_tok, d_model)
    normed = rms_norm(x_flat).astype(jnp.bfloat16)
    project = lambda w: jnp.dot(normed, w, preferred_element_type=jnp.float32).astype(jnp.bfloat16)
    q, k, v = project(w_q), project(w_k), project(w_v)

    halves = []
    for s in range(n_seq):
        o = attention(q, k, v, s, seq, head)
        attn = jnp.dot(o, w_o, preferred_element_type=jnp.float32).astype(jnp.bfloat16)
        h = (x_loc[s].astype(jnp.float32) + attn.astype(jnp.float32)).astype(jnp.bfloat16)
        r = rms_norm(h)
        u = r.astype(jnp.bfloat16)
        u_rows = u.reshape(seq, SUB, LANES)
        logits = jnp.dot(r, w_router, precision=lax.Precision.HIGHEST, preferred_element_type=jnp.float32)
        ids_s = lax.slice_in_dim(ids, s * seq, (s + 1) * seq)
        hit = ids_s[:, :, None] == lax.broadcasted_iota(jnp.int32, (1, 1, n_exp), 2)
        chosen = jnp.sum(jnp.where(hit, logits[:, None, :], 0.0), axis=-1)
        gates = jnp.pad(jax.nn.softmax(chosen, axis=-1), ((0, 0), (0, 8 - top)))
        u_x, g_x = over_x(u_rows), over_x(gates)
        u_c, g_c = over_core(u_rows), over_core(gates)
        u_d, g_d = over_core(u_x), over_core(g_x)
        halves.append((h, u, u_rows, gates, u_x, g_x, u_c, g_c, u_d, g_d))

    sums = [None] * n_seq

    def run(s, remote):
        h, u, u_rows, gates, u_x, g_x, u_c, g_c, u_d, g_d = halves[s]
        if remote:
            toks, bounds = plan_of(me ^ 2, me ^ 3, s)
            args = jnp.concatenate([g_x, g_d]).reshape(-1), u_x, u_d
        else:
            toks, bounds = plan_of(me, me ^ 1, s)
            args = jnp.concatenate([gates, g_c]).reshape(-1), u_rows, u_c
        mine, theirs = expert_pass(toks, bounds, *args, w_gate, w_up, w_down, n_key, "remote" if remote else "local")
        total = mine + over_core(theirs)
        return over_x(total) if remote else total

    far = [run(s, True) for s in range(n_seq)]
    near = [run(s, False) for s in range(n_seq)]

    s_gate, s_up = gather_weight(sgate_shard, 0), gather_weight(sup_shard, 0)
    s_down = gather_weight(sdown_shard, 1)
    u = jnp.concatenate([half[1] for half in halves])
    gate_act = jnp.dot(u, s_gate, preferred_element_type=jnp.float32)
    up_act = jnp.dot(u, s_up, preferred_element_type=jnp.float32)
    middle = (jax.nn.silu(gate_act) * up_act).astype(jnp.bfloat16)
    shared = jnp.dot(middle, s_down, preferred_element_type=jnp.float32).astype(jnp.bfloat16)
    out = []
    for s in range(n_seq):
        routed = (near[s] + far[s]).reshape(seq, d_model)
        part = lax.slice_in_dim(shared, s * seq, (s + 1) * seq).astype(jnp.float32)
        out.append((halves[s][0].astype(jnp.float32) + routed + part).astype(jnp.bfloat16))
    return jnp.stack(out)


def solution(mesh):
    tok_spec = P(("dp", "ep"), None, None)
    row_spec = P("ep", None)
    cube_spec = P("ep", None, None)
    in_specs = (tok_spec, cube_spec, cube_spec, cube_spec, row_spec, P(None, None), cube_spec, cube_spec, cube_spec, row_spec, row_spec, row_spec, tok_spec)
    return jax.shard_map(local_layer, mesh=mesh, in_specs=in_specs, out_specs=tok_spec, check_vma=False)
```
